32 devices in a mesh: row: 4 (over y, x), col: 2 (over core), layer: 4 (over z).
Axes of the slice: x: 2, y: 2, z: 4, core: 2. Of those that a mesh axis runs over, the one named last changes fastest.
Arguments:
- matrix: float32 [4096, 4096], P('row', 'col'), may hold values from -6 to 6
- pattern: int32 [128, 128], P('row', 'col'), may hold values 0 or 1
- keep: int32 [128, 128], P('row', 'col'), may hold values 0 or 1
Outputs:
- update: float32 [4096, 4096], P(('row', 'layer'), 'col')
The draws below stay inside these ranges and needn't reach their ends.
All inputs are finite; a program needn't handle non-finite values. No bound on the sum of `pattern` or of `keep` on one device may be relied on, other than what follows from the above.
Results may differ from the reference program's by a relative error of at most 0.00005.
Values sent between devices are 32-bit elements; how exact they have to be, the bound alone decides.
A program may use at most 128 MiB of HBM per device.

```python
import jax
import jax.numpy as jnp
from jax import lax

BS = 32
NB = 128
ORDER = 4096


def plant(entries, key, low, largest):
    longest = entries.shape.index(max(entries.shape))
    spots = []
    for shift in (0, 1):
        where = [jax.random.randint(jax.random.fold_in(key, axis), (), 0, length) for axis, length in enumerate(entries.shape)]
        where[longest] = (where[longest] + shift) % entries.shape[longest]
        spots.append(tuple(where))
    return entries.at[spots[0]].set(low).at[spots[1]].set(largest)


def shard_levels(rng, dims, shards, low, largest):
    def one(axis_at, blocks):
        steps = jax.random.uniform(jax.random.fold_in(jax.random.fold_in(rng, 6), axis_at), (blocks,), jnp.float32, low / len(shards), largest / len(shards))
        return jnp.repeat(jnp.exp(steps), dims[axis_at] // blocks).reshape((-1,) + (1,) * (len(dims) - axis_at - 1))

    gain = one(*shards[0])
    for cut in shards[1:]:
        gain = gain * one(*cut)
    return gain


def normal_values(key, shape, deviation, limit, shards=(), kind=jnp.bfloat16):
    entries = deviation * jax.random.normal(key, shape, jnp.float32)
    if shards:
        entries = entries * shard_levels(key, shape, shards, -0.22, 0.18)
    return jnp.clip(entries, -limit, limit).astype(kind)


def setup_inputs(seed: int = 0) -> dict:
    streams_of = jax.random.split(jax.random.key(seed), 4)
    return {
        "matrix": normal_values(streams_of[0], (ORDER, ORDER), 1.0, 6.0, ((0, 4), (1, 2)), jnp.float32),
        "pattern": plant((jax.random.randint(streams_of[1], (NB, NB), 0, 2) < 1).astype(jnp.int32), jax.random.fold_in(streams_of[1], 1), 0, 1),
        "keep": plant((jax.random.randint(streams_of[2], (NB, NB), 0, 4) < 3).astype(jnp.int32), jax.random.fold_in(streams_of[2], 1), 0, 1),
    }


def blockwise(values, flags):
    shaped = values.reshape(NB, BS, NB, BS) * flags.astype(jnp.float32)[:, None, :, None]
    return shaped.reshape(NB * BS, NB * BS)


def reference(matrix, pattern, keep):
    sparse = blockwise(matrix, pattern)
    square = jnp.dot(sparse, sparse, preferred_element_type=jnp.float32, precision=lax.Precision.HIGHEST)
    filtered = blockwise(square, keep)
    product = jnp.dot(sparse, filtered, preferred_element_type=jnp.float32, precision=lax.Precision.HIGHEST)
    factor = 0.72 / (NB * BS)
    return 1.5 * sparse - (0.5 * factor) * product
```

```python
import functools

import jax
import jax.numpy as jnp
from jax import lax
from jax.experimental import pallas as pl
from jax.experimental.pallas import tpu as pltpu
from jax.sharding import PartitionSpec as P

MESH = pl.DeviceIdType.MESH
LANES = 128
DAMPING = 0.72


def masked(values, flags):
    rows, cols = values.shape
    block_rows, block_cols = flags.shape
    shaped = values.reshape(block_rows, rows // block_rows, block_cols, cols // block_cols)
    return (shaped * flags.astype(jnp.float32)[:, None, :, None]).reshape(rows, cols)


def plain(matrix, pattern, keep):
    rows, cols = matrix.shape
    layers = lax.axis_size("layer")
    level = lax.axis_index("layer")
    width = cols // layers
    flags = pattern.shape[1] // layers
    sparse = masked(matrix, pattern)
    left = lax.all_gather(sparse, "col", axis=1, tiled=True)
    mine = lax.dynamic_slice_in_dim(sparse, level * width, width, 1)
    right = lax.all_gather(mine, "row", axis=0, tiled=True)
    multiply = functools.partial(
        jnp.dot, preferred_element_type=jnp.float32, precision=lax.Precision.HIGH
    )
    filtered = masked(
        multiply(left, right), lax.dynamic_slice_in_dim(keep, level * flags, flags, 1)
    )
    product = multiply(left, lax.all_gather(filtered, "row", axis=0, tiled=True))
    factor = DAMPING / (rows * lax.axis_size("row"))
    update = 1.5 * mine - 0.5 * factor * product
    return lax.all_to_all(update, "layer", split_axis=0, concat_axis=1, tiled=True)


def split(values):
    high = values.astype(jnp.bfloat16)
    low = (values - high.astype(jnp.float32)).astype(jnp.bfloat16)
    return high, low


def kernel(
    layers, block, factor,
    matrix, pattern, keep, out,
    raw, panel, a_high, a_low, both, total, staged, flags_in, flags_a, flags_x, flags_keep,
    send_sem, recv_sem, panel_send, panel_recv, flag_send, flag_recv, out_send, out_recv, local_sem,
):
    rows, cols = matrix.shape
    chunks = cols // layers // LANES
    tasks = 2 * chunks
    half = rows // 2
    share = rows // layers
    block_rows = rows // block
    row = lax.axis_index("row")
    col = lax.axis_index("col")
    level = lax.axis_index("layer")
    y, x = row // 2, row % 2
    along_x = {"row": y * 2 + (1 - x)}
    along_y = {"row": (1 - y) * 2 + x}
    across = {"row": (1 - y) * 2 + (1 - x)}
    twin = {"col": 1 - col}
    others = [{"layer": (level + step) % layers} for step in range(1, layers)]

    barrier = pltpu.get_barrier_semaphore()
    peers = [along_x, along_y, across, twin] + others
    for peer in peers:
        pl.semaphore_signal(barrier, inc=1, device_id=peer, device_id_type=MESH)
    pl.semaphore_wait(barrier, len(peers))

    def remote(source, target, sent, landed, peer):
        return pltpu.make_async_remote_copy(
            src_ref=source, dst_ref=target, send_sem=sent, recv_sem=landed,
            device_id=peer, device_id_type=MESH,
        )

    def part(task, slot, top):
        return raw.at[task, slot, pl.ds(top * half, half)]

    def move(task, arrival, source):
        slot, top = ((1, 0), (1, 1), (2, 1), (2, 0), (3, 0), (3, 1))[arrival]
        peer = along_x if arrival in (0, 1, 5) else along_y
        return remote(
            source, part(task, slot, top), send_sem.at[task, arrival], recv_sem.at[task, arrival], peer
        )

    def own_x(task, top):
        start = pl.multiple_of((level * chunks + task) * LANES, LANES)
        return matrix.at[pl.ds(top * half, half), pl.ds(start, LANES)]

    def send_x(task):
        for arrival, top in ((0, 0), (2, 1), (1, 1), (3, 0)):
            move(task, arrival, own_x(task, top)).start()

    def send_f(task):
        for arrival, top in ((0, 0), (2, 1), (1, 1), (3, 0)):
            move(task, arrival, part(task, 0, top)).start()

    def hand_on(task):
        move(task, 0, part(task, 1, 0)).wait_recv()
        move(task, 4, part(task, 1, 0)).start()
        move(task, 2, part(task, 2, 1)).wait_recv()
        move(task, 5, part(task, 2, 1)).start()

    send_x(0)

    flag_moves = [
        remote(pattern, flags_in.at[n], flag_send.at[n], flag_recv.at[n], peer)
        for n, peer in enumerate((along_x, along_y, across, twin))
    ]
    for copy in flag_moves:
        copy.start()
    bands = 4
    tall = rows // bands

    def band(n):
        return pl.ds(n * tall, tall)

    panel_moves = [
        remote(matrix.at[band(n)], panel.at[1, band(n)], panel_send.at[n], panel_recv.at[n], twin)
        for n in range(bands)
    ]
    panel_local = [
        pltpu.make_async_copy(matrix.at[band(n)], panel.at[0, band(n)], local_sem.at[n])
        for n in range(bands)
    ]
    piece_local = [
        pltpu.make_async_copy(
            matrix.at[:, pl.ds(pl.multiple_of((level * chunks + n) * LANES, LANES), LANES)],
            raw.at[n, 0],
            local_sem.at[bands + n],
        )
        for n in range(chunks)
    ]
    for n in range(bands):
        panel_local[n].start()
        panel_moves[n].start()
    for copy in piece_local:
        copy.start()

    def expand(flags, first, width):
        index = lax.broadcasted_iota(jnp.int32, (flags.shape[1], width), 0)
        lane = lax.broadcasted_iota(jnp.int32, (flags.shape[1], width), 1)
        start = (index - first) * block
        table = jnp.where((lane >= start) & (lane < start + block), 1.0, 0.0)
        return jnp.dot(
            flags.astype(jnp.bfloat16), table.astype(jnp.bfloat16), preferred_element_type=jnp.float32
        )

    per_chunk = LANES // block

    def expand_chunks(flags, store):
        for n in range(chunks):
            store(n, expand(flags, (level * chunks + n) * per_chunk, LANES))

    def store_x(slot):
        def store(n, values):
            flags_x[n, slot] = values
        return store

    def store_keep(n, values):
        flags_keep[n] = values

    group = 8

    def prepare_panel(side, owner_col):
        for n in range(cols // half):
            owner = owner_col * (cols // rows) + n // 2
            slot = (owner // 2 + y) % 2 * 2 + (owner % 2 + x) % 2
            place = slot * 2 + n % 2

            def body(i, carry):
                flags = flags_a[side, pl.ds(pl.multiple_of(i * group, group), group), n * half : (n + 1) * half]
                for b in range(group):
                    at = pl.ds(pl.multiple_of((i * group + b) * block, block), block)
                    values = panel[side, at, n * half : (n + 1) * half] * flags[b : b + 1]
                    high, low = split(values)
                    a_high[place, at] = high
                    a_low[place, at] = low
                return carry

            lax.fori_loop(0, block_rows // group, body, 0)

    def take(task, slot, top):
        which = task - (task // chunks) * (task - chunks)

        def convert(i, carry):
            first = top * (half // block) + i * group
            flags = flags_x[which, slot, pl.ds(pl.multiple_of(first, group), group), :]
            for b in range(group):
                at = pl.ds(pl.multiple_of((first + b) * block, block), block)
                to = pl.ds(pl.multiple_of((i * group + b) * block, block), block)
                high, low = split(raw[task, slot, at, :] * flags[b : b + 1])
                both[to, 0:LANES] = high
                both[to, LANES : 2 * LANES] = low
            return carry

        lax.fori_loop(0, half // block // group, convert, 0)
        place = slot * 2 + top

        def multiply(i, carry):
            at = pl.ds(pl.multiple_of(i * half, half), half)
            total[at, :] += jnp.dot(
                a_high[place, at, :], both[...], preferred_element_type=jnp.float32
            ) + jnp.dot(a_low[place, at, :], both[...], preferred_element_type=jnp.float32)
            return carry

        lax.fori_loop(0, 2, multiply, 0)

    def finish(task):
        total[...] = jnp.zeros_like(total)

        def present(g, carry):
            take(task, g // 2 * (1 + g % 2), g % 2)
            return carry

        lax.fori_loop(0, 4, present, 0)
        for arrival, slot, top in ((3, 2, 0), (1, 1, 1), (4, 3, 0), (5, 3, 1)):
            move(task, arrival, part(task, slot, top)).wait_recv()
            if arrival == 1:
                late(task, 0)
            if arrival == 5:
                late(task, 2)

    def late(task, base):
        def body(g, carry):
            take(task, (1 - base // 2) * (2 - g) + base // 2 * 3, g)
            return carry

        lax.fori_loop(0, 2, body, 0)

    def block_loop(body):
        def step(i, carry):
            for b in range(group):
                body(i, b)
            return carry

        lax.fori_loop(0, block_rows // group, step, 0)

    def at_block(i, b):
        return pl.ds(pl.multiple_of((i * group + b) * block, block), block)

    def finish_square(task):
        finish(task)

        def body(i, b):
            flags = flags_keep[task, pl.ds(pl.multiple_of(i * group, group), group), :]
            at = at_block(i, b)
            summed = total[at, 0:LANES] + total[at, LANES : 2 * LANES]
            raw[task + chunks, 0, at, :] = summed * flags[b : b + 1]

        block_loop(body)

    def out_move(n, step):
        target = (level + step) % layers
        start = pl.multiple_of((level * chunks + n) * LANES, LANES)
        return remote(
            staged.at[n, pl.ds(pl.multiple_of(target * share, share), share)],
            out.at[:, pl.ds(start, LANES)],
            out_send.at[n, step - 1],
            out_recv.at[n, step - 1],
            {"layer": target},
        )

    def out_local(n):
        start = pl.multiple_of((level * chunks + n) * LANES, LANES)
        return pltpu.make_async_copy(
            staged.at[n, pl.ds(pl.multiple_of(level * share, share), share)],
            out.at[:, pl.ds(start, LANES)],
            local_sem.at[bands + chunks + n],
        )

    def finish_update(task):
        finish(task)
        n = task - chunks

        def body(i, b):
            flags = flags_x[n, 0, pl.ds(pl.multiple_of(i * group, group), group), :]
            at = at_block(i, b)
            summed = total[at, 0:LANES] + total[at, LANES : 2 * LANES]
            staged[n, at, :] = 1.5 * (raw[n, 0, at, :] * flags[b : b + 1]) - factor * summed

        block_loop(body)
        for step in range(1, layers):
            out_move(n, step).start()
        out_local(n).start()

    flags_a[0] = expand(pattern[...], 0, cols)
    expand_chunks(pattern[...], store_x(0))
    expand_chunks(keep[...], store_keep)
    flags_x[chunks] = jnp.ones_like(flags_x[chunks])
    for copy in panel_local:
        copy.wait()
    prepare_panel(0, col)
    for copy in piece_local:
        copy.wait()

    hand_on(0)
    send_x(1)
    for copy in flag_moves:
        copy.wait_recv()
    flags_a[1] = expand(flags_in[3], 0, cols)
    for slot in (1, 2, 3):
        expand_chunks(flags_in[slot - 1], store_x(slot))
    for copy in panel_moves:
        copy.wait_recv()
    prepare_panel(1, 1 - col)

    def advance(task, carry):
        @pl.when(task < tasks)
        def _():
            hand_on(task)

        @pl.when(task + 1 < chunks)
        def _():
            send_x(task + 1)

        @pl.when((task + 1 >= chunks) & (task + 1 < tasks))
        def _():
            send_f(task + 1)

        @pl.when(task - 1 < chunks)
        def _():
            finish_square(task - 1)

        @pl.when(task - 1 >= chunks)
        def _():
            finish_update(task - 1)

        return carry

    lax.fori_loop(1, tasks + 1, advance, 0)

    for copy in flag_moves + panel_moves:
        copy.wait_send()

    def drain(task, carry):
        for arrival in range(6):
            move(task, arrival, part(task, 0, 0)).wait_send()
        return carry

    lax.fori_loop(0, tasks, drain, 0)

    def drain_out(n, carry):
        for step in range(1, layers):
            out_move(n, step).wait()
        out_local(n).wait()
        return carry

    lax.fori_loop(0, chunks, drain_out, 0)


def fused(matrix, pattern, keep):
    rows, cols = matrix.shape
    layers = lax.axis_size("layer")
    block_rows, block_cols = pattern.shape
    block = rows // block_rows
    chunks = cols // layers // LANES
    tasks = 2 * chunks
    half = rows // 2
    wide = -(-block_cols // LANES) * LANES
    factor = 0.5 * DAMPING / (rows * lax.axis_size("row"))

    def padded(flags):
        return jnp.pad(flags.astype(jnp.float32), ((0, 0), (0, wide - block_cols)))

    vmem = pl.BlockSpec(memory_space=pltpu.VMEM)
    anywhere = pl.BlockSpec(memory_space=pl.ANY)
    dma = pltpu.SemaphoreType.DMA
    return pl.pallas_call(
        functools.partial(kernel, layers, block, factor),
        out_shape=jax.ShapeDtypeStruct((rows // layers, cols), jnp.float32),
        in_specs=[anywhere, vmem, vmem],
        out_specs=anywhere,
        scratch_shapes=[
            pltpu.VMEM((tasks, 4, rows, LANES), jnp.float32),
            pltpu.VMEM((2, rows, cols), jnp.float32),
            pltpu.VMEM((8, rows, half), jnp.bfloat16),
            pltpu.VMEM((8, rows, half), jnp.bfloat16),
            pltpu.VMEM((half, 2 * LANES), jnp.bfloat16),
            pltpu.VMEM((rows, 2 * LANES), jnp.float32),
            pltpu.VMEM((chunks, rows, LANES), jnp.float32),
            pltpu.VMEM((4, block_rows, wide), jnp.float32),
            pltpu.VMEM((2, block_rows, cols), jnp.float32),
            pltpu.VMEM((chunks + 1, 4, block_rows, LANES), jnp.float32),
            pltpu.VMEM((chunks, block_rows, LANES), jnp.float32),
            dma((tasks, 6)),
            dma((tasks, 6)),
            dma((4,)),
            dma((4,)),
            dma((4,)),
            dma((4,)),
            dma((chunks, max(layers - 1, 1))),
            dma((chunks, max(layers - 1, 1))),
            dma((4 + 2 * chunks,)),
        ],
        compiler_params=pltpu.CompilerParams(
            collective_id=0, has_side_effects=True, vmem_limit_bytes=67_000_000
        ),
    )(matrix, padded(pattern), padded(keep))


def local(matrix, pattern, keep):
    rows, cols = matrix.shape
    layers = lax.axis_size("layer")
    block = rows // pattern.shape[0]
    fits = (
        lax.axis_size("row") == 4
        and lax.axis_size("col") == 2
        and cols % (layers * LANES) == 0
        and cols // (layers * LANES) >= 3
        and LANES % block == 0
        and block % 16 == 0
        and rows % (16 * block) == 0
        and rows % (8 * layers) == 0
        and (rows // 2) % LANES == 0
        and rows * cols <= 1 << 21
    )
    return (fused if fits else plain)(matrix, pattern, keep)


def solution(mesh):
    placed = (P("row", "col"), P("row", "col"), P("row", "col"))
    return jax.shard_map(
        local, mesh=mesh, in_specs=placed, out_specs=P(("row", "layer"), "col"), check_vma=False
    )
```

```python
import functools

import jax
import jax.numpy as jnp
from jax import lax
from jax.experimental import pallas as pl
from jax.experimental.pallas import tpu as pltpu
from jax.sharding import PartitionSpec as P

MESH = pl.DeviceIdType.MESH
LANES = 128
DAMPING = 0.72


def masked(values, flags):
    rows, cols = values.shape
    block_rows, block_cols = flags.shape
    shaped = values.reshape(block_rows, rows // block_rows, block_cols, cols // block_cols)
    return (shaped * flags.astype(jnp.float32)[:, None, :, None]).reshape(rows, cols)


def plain(matrix, pattern, keep):
    rows, cols = matrix.shape
    layers = lax.axis_size("layer")
    level = lax.axis_index("layer")
    width = cols // layers
    flags = pattern.shape[1] // layers
    sparse = masked(matrix, pattern)
    left = lax.all_gather(sparse, "col", axis=1, tiled=True)
    mine = lax.dynamic_slice_in_dim(sparse, level * width, width, 1)
    right = lax.all_gather(mine, "row", axis=0, tiled=True)
    multiply = functools.partial(
        jnp.dot, preferred_element_type=jnp.float32, precision=lax.Precision.HIGH
    )
    filtered = masked(
        multiply(left, right), lax.dynamic_slice_in_dim(keep, level * flags, flags, 1)
    )
    product = multiply(left, lax.all_gather(filtered, "row", axis=0, tiled=True))
    factor = DAMPING / (rows * lax.axis_size("row"))
    update = 1.5 * mine - 0.5 * factor * product
    return lax.all_to_all(update, "layer", split_axis=0, concat_axis=1, tiled=True)


def split(values):
    high = values.astype(jnp.bfloat16)
    low = (values - high.astype(jnp.float32)).astype(jnp.bfloat16)
    return high, low


def kernel(
    layers, block, factor,
    matrix, pattern, keep, out,
    raw, panel, a_high, a_low, both, total, staged, flags_in, flags_a, flags_x, flags_keep,
    send_sem, recv_sem, panel_send, panel_recv, flag_send, flag_recv, out_send, out_recv, local_sem,
):
    rows, cols = matrix.shape
    chunks = cols // layers // LANES
    tasks = 2 * chunks
    half = rows // 2
    share = rows // layers
    block_rows = rows // block
    row = lax.axis_index("row")
    col = lax.axis_index("col")
    level = lax.axis_index("layer")
    y, x = row // 2, row % 2
    along_x = {"row": y * 2 + (1 - x)}
    along_y = {"row": (1 - y) * 2 + x}
    across = {"row": (1 - y) * 2 + (1 - x)}
    twin = {"col": 1 - col}
    others = [{"layer": (level + step) % layers} for step in range(1, layers)]

    barrier = pltpu.get_barrier_semaphore()
    peers = [along_x, along_y, across, twin] + others
    for peer in peers:
        pl.semaphore_signal(barrier, inc=1, device_id=peer, device_id_type=MESH)
    pl.semaphore_wait(barrier, len(peers))

    def remote(source, target, sent, landed, peer):
        return pltpu.make_async_remote_copy(
            src_ref=source, dst_ref=target, send_sem=sent, recv_sem=landed,
            device_id=peer, device_id_type=MESH,
        )

    def part(task, slot, top):
        return raw.at[task, slot, pl.ds(top * half, half)]

    def move(task, arrival, source):
        slot, top = ((1, 0), (1, 1), (2, 1), (2, 0), (3, 0), (3, 1))[arrival]
        peer = along_x if arrival in (0, 1, 5) else along_y
        return remote(
            source, part(task, slot, top), send_sem.at[task, arrival], recv_sem.at[task, arrival], peer
        )

    def own_x(task, top):
        start = pl.multiple_of((level * chunks + task) * LANES, LANES)
        return matrix.at[pl.ds(top * half, half), pl.ds(start, LANES)]

    def send_x(task):
        for arrival, top in ((0, 0), (2, 1), (1, 1), (3, 0)):
            move(task, arrival, own_x(task, top)).start()

    def send_f(task):
        for arrival, top in ((0, 0), (2, 1), (1, 1), (3, 0)):
            move(task, arrival, part(task, 0, top)).start()

    def hand_on(task):
        move(task, 0, part(task, 1, 0)).wait_recv()
        move(task, 4, part(task, 1, 0)).start()
        move(task, 2, part(task, 2, 1)).wait_recv()
        move(task, 5, part(task, 2, 1)).start()

    @pl.when(col == 0)
    def _():
        send_x(0)

    flag_moves = [
        remote(pattern, flags_in.at[n], flag_send.at[n], flag_recv.at[n], peer)
        for n, peer in enumerate((along_x, along_y, across, twin))
    ]
    for copy in flag_moves:
        copy.start()
    bands = 4
    tall = rows // bands

    def band(n):
        return pl.ds(n * tall, tall)

    panel_moves = [
        remote(matrix.at[band(n)], panel.at[band(n)], panel_send.at[n], panel_recv.at[n], twin)
        for n in range(bands)
    ]
    def own_panel(n):
        return raw.at[chunks + n // 4, n % 4]

    panel_local = [
        pltpu.make_async_copy(
            matrix.at[:, pl.ds(n * LANES, LANES)], own_panel(n), local_sem.at[2 * chunks + n]
        )
        for n in range(cols // LANES)
    ]
    piece_local = [
        pltpu.make_async_copy(
            matrix.at[:, pl.ds(pl.multiple_of((level * chunks + n) * LANES, LANES), LANES)],
            raw.at[n, 0],
            local_sem.at[n],
        )
        for n in range(chunks)
    ]
    for copy in panel_moves + panel_local + piece_local:
        copy.start()

    def expand(flags, first, width):
        index = lax.broadcasted_iota(jnp.int32, (flags.shape[1], width), 0)
        lane = lax.broadcasted_iota(jnp.int32, (flags.shape[1], width), 1)
        start = (index - first) * block
        table = jnp.where((lane >= start) & (lane < start + block), 1.0, 0.0)
        return jnp.dot(
            flags.astype(jnp.float32).astype(jnp.bfloat16), table.astype(jnp.bfloat16), preferred_element_type=jnp.float32
        )

    per_chunk = LANES // block

    def expand_chunks(flags, store):
        for n in range(chunks):
            store(n, expand(flags, (level * chunks + n) * per_chunk, LANES))

    def store_x(slot):
        def store(n, values):
            flags_x[n, slot] = values
        return store

    def store_keep(n, values):
        flags_keep[n] = values

    group = 8

    def prepare_panel(side, owner_col):
        for n in range(cols // half):
            owner = owner_col * (cols // rows) + n // 2
            slot = (owner // 2 + y) % 2 * 2 + (owner % 2 + x) % 2
            place = slot * 2 + n % 2

            def body(i, carry):
                base = pl.multiple_of(i * group, group)
                for m in range(half // LANES):
                    lanes = n * half + m * LANES
                    flags = flags_a[side, pl.ds(base, group), lanes : lanes + LANES]
                    for b in range(group):
                        at = pl.ds(pl.multiple_of((i * group + b) * block, block), block)
                        if side:
                            values = panel[at, lanes : lanes + LANES]
                        else:
                            values = own_panel(lanes // LANES)[at, :]
                        high, low = split(values * flags[b : b + 1])
                        a_high[place, at, m * LANES : (m + 1) * LANES] = high
                        a_low[place, at, m * LANES : (m + 1) * LANES] = low
                return carry

            lax.fori_loop(0, block_rows // group, body, 0)

    def at_block(i, b):
        return pl.ds(pl.multiple_of((i * group + b) * block, block), block)

    def convert(task, slot, top):
        which = task - (task // chunks) * (task - chunks)

        def body(i, carry):
            flags = flags_x[which, slot, pl.ds(pl.multiple_of(i * group, group), group), :]
            for b in range(group):
                at = at_block(i, b)
                high, low = split(raw[task, slot, at, :] * flags[b : b + 1])
                both[at, 0:LANES] = high
                both[at, LANES : 2 * LANES] = low
            return carry

        steps = block_rows // group // 2
        lax.fori_loop(top * steps, (top + 1) * steps, body, 0)

    def out_move(n, step):
        target = (level + step) % layers
        start = pl.multiple_of((level * chunks + n) * LANES, LANES)
        return remote(
            staged.at[n, pl.ds(pl.multiple_of(target * share, share), share)],
            out.at[:, pl.ds(start, LANES)],
            out_send.at[n, step - 1],
            out_recv.at[n, step - 1],
            {"layer": target},
        )

    def out_local(n):
        start = pl.multiple_of((level * chunks + n) * LANES, LANES)
        return pltpu.make_async_copy(
            staged.at[n, pl.ds(pl.multiple_of(level * share, share), share)],
            out.at[:, pl.ds(start, LANES)],
            local_sem.at[chunks + n],
        )

    def finish_rows(task, tile):
        steps = block_rows // group // 2

        def square(i, carry):
            flags = flags_keep[task, pl.ds(pl.multiple_of(i * group, group), group), :]
            for b in range(group):
                at = at_block(i, b)
                summed = total[at, 0:LANES] + total[at, LANES : 2 * LANES]
                raw[task + chunks, 0, at, :] = summed * flags[b : b + 1]
            return carry

        def update(i, carry):
            n = task - chunks
            flags = flags_x[n, 0, pl.ds(pl.multiple_of(i * group, group), group), :]
            for b in range(group):
                at = at_block(i, b)
                summed = total[at, 0:LANES] + total[at, LANES : 2 * LANES]
                staged[n, at, :] = 1.5 * (raw[n, 0, at, :] * flags[b : b + 1]) - factor * summed
            return carry

        @pl.when(task < chunks)
        def _():
            lax.fori_loop(tile * steps, (tile + 1) * steps, square, 0)

        @pl.when(task >= chunks)
        def _():
            lax.fori_loop(tile * steps, (tile + 1) * steps, update, 0)

    def finish(task):
        total[...] = jnp.zeros_like(total)

        def pair(g, carry):
            other = g % 2 * 2 + g // 2

            @pl.when(g >= 2)
            def _():
                for slot, top, arrival in ((g, 0, g + 1), (other, 1, 4 * g - 7)):
                    remote(
                        part(task, slot, top), part(task, slot, top),
                        send_sem.at[task, arrival], recv_sem.at[task, arrival], along_x,
                    ).wait_recv()

            convert(task, g, 0)
            convert(task, other, 1)

            def multiply(tile, carry):
                at = pl.ds(pl.multiple_of(tile * half, half), half)
                value = total[at, :]
                for place, rows_of in ((g * 2, both.at[0:half]), (other * 2 + 1, both.at[half:rows])):
                    for side in (a_high, a_low):
                        value += jnp.dot(
                            side[place, at, :], rows_of[...], preferred_element_type=jnp.float32
                        )
                total[at, :] = value

                @pl.when(g == 3)
                def _():
                    finish_rows(task, tile)

                return carry

            lax.fori_loop(0, 2, multiply, 0)
            return carry

        lax.fori_loop(0, 4, pair, 0)

        @pl.when(task >= chunks)
        def _():
            for step in range(1, layers):
                out_move(task - chunks, step).start()
            out_local(task - chunks).start()

    def prepare_own():
        for copy in panel_local:
            copy.wait()
        prepare_panel(0, col)

    def send(task):
        @pl.when(task < chunks)
        def _():
            send_x(task)

        @pl.when((task >= chunks) & (task < tasks))
        def _():
            send_f(task)

    flags_a[0] = expand(pattern[...], 0, cols)

    @pl.when(col == 1)
    def _():
        prepare_own()
        send_x(0)

    expand_chunks(pattern[...], store_x(0))
    expand_chunks(keep[...], store_keep)
    flags_x[chunks] = jnp.ones_like(flags_x[chunks])
    for copy in piece_local:
        copy.wait()

    hand_on(0)
    send_x(1)

    @pl.when(col == 0)
    def _():
        prepare_own()

    for copy in flag_moves:
        copy.wait_recv()
    flags_a[1] = expand(flags_in[3], 0, cols)
    for slot in (1, 2, 3):
        expand_chunks(flags_in[slot - 1], store_x(slot))
    for copy in panel_moves:
        copy.wait_recv()
    prepare_panel(1, 1 - col)
    finish(0)

    def advance(task, carry):
        hand_on(task)
        send(task + 1)
        finish(task)
        return carry

    lax.fori_loop(1, tasks, advance, 0)

    for copy in flag_moves + panel_moves:
        copy.wait_send()

    def drain(task, carry):
        for arrival in range(6):
            move(task, arrival, part(task, 0, 0)).wait_send()
        return carry

    lax.fori_loop(0, tasks, drain, 0)

    def drain_out(n, carry):
        for step in range(1, layers):
            out_move(n, step).wait()
        out_local(n).wait()
        return carry

    lax.fori_loop(0, chunks, drain_out, 0)


def fused(matrix, pattern, keep):
    rows, cols = matrix.shape
    layers = lax.axis_size("layer")
    block_rows, block_cols = pattern.shape
    block = rows // block_rows
    chunks = cols // layers // LANES
    tasks = 2 * chunks
    half = rows // 2
    factor = 0.5 * DAMPING / (rows * lax.axis_size("row"))

    vmem = pl.BlockSpec(memory_space=pltpu.VMEM)
    anywhere = pl.BlockSpec(memory_space=pl.ANY)
    dma = pltpu.SemaphoreType.DMA
    return pl.pallas_call(
        functools.partial(kernel, layers, block, factor),
        out_shape=jax.ShapeDtypeStruct((rows // layers, cols), jnp.float32),
        in_specs=[anywhere, vmem, vmem],
        out_specs=vmem,
        scratch_shapes=[
            pltpu.VMEM((tasks, 4, rows, LANES), jnp.float32),
            pltpu.VMEM((rows, cols), jnp.float32),
            pltpu.VMEM((8, rows, half), jnp.bfloat16),
            pltpu.VMEM((8, rows, half), jnp.bfloat16),
            pltpu.VMEM((rows, 2 * LANES), jnp.bfloat16),
            pltpu.VMEM((rows, 2 * LANES), jnp.float32),
            pltpu.VMEM((chunks, rows, LANES), jnp.float32),
            pltpu.VMEM((4, block_rows, block_cols), jnp.int32),
            pltpu.VMEM((2, block_rows, cols), jnp.float32),
            pltpu.VMEM((chunks + 1, 4, block_rows, LANES), jnp.float32),
            pltpu.VMEM((chunks, block_rows, LANES), jnp.float32),
            dma((tasks, 6)),
            dma((tasks, 6)),
            dma((4,)),
            dma((4,)),
            dma((4,)),
            dma((4,)),
            dma((chunks, max(layers - 1, 1))),
            dma((chunks, max(layers - 1, 1))),
            dma((2 * chunks + cols // LANES,)),
        ],
        compiler_params=pltpu.CompilerParams(
            collective_id=0, has_side_effects=True, vmem_limit_bytes=52_000_000
        ),
    )(matrix, pattern, keep)


def local(matrix, pattern, keep):
    rows, cols = matrix.shape
    layers = lax.axis_size("layer")
    block = rows // pattern.shape[0]
    fits = (
        lax.axis_size("row") == 4
        and lax.axis_size("col") == 2
        and cols % (layers * LANES) == 0
        and cols // (layers * LANES) >= 3
        and LANES % block == 0
        and block % 16 == 0
        and rows % (16 * block) == 0
        and rows % (8 * layers) == 0
        and (rows // 2) % LANES == 0
        and rows * cols <= 1 << 21
        and layers <= 4
    )
    return (fused if fits else plain)(matrix, pattern, keep)


def solution(mesh):
    placed = (P("row", "col"), P("row", "col"), P("row", "col"))
    return jax.shard_map(
        local, mesh=mesh, in_specs=placed, out_specs=P(("row", "layer"), "col"), check_vma=False
    )
```

```python
import functools

import jax
import jax.numpy as jnp
from jax import lax
from jax.experimental import pallas as pl
from jax.experimental.pallas import tpu as pltpu
from jax.sharding import PartitionSpec as P

MESH = pl.DeviceIdType.MESH
LANES = 128
DAMPING = 0.72


def masked(values, flags):
    rows, cols = values.shape
    block_rows, block_cols = flags.shape
    shaped = values.reshape(block_rows, rows // block_rows, block_cols, cols // block_cols)
    return (shaped * flags.astype(jnp.float32)[:, None, :, None]).reshape(rows, cols)


def plain(matrix, pattern, keep):
    rows, cols = matrix.shape
    layers = lax.axis_size("layer")
    level = lax.axis_index("layer")
    width = cols // layers
    flags = pattern.shape[1] // layers
    sparse = masked(matrix, pattern)
    left = lax.all_gather(sparse, "col", axis=1, tiled=True)
    mine = lax.dynamic_slice_in_dim(sparse, level * width, width, 1)
    right = lax.all_gather(mine, "row", axis=0, tiled=True)
    multiply = functools.partial(
        jnp.dot, preferred_element_type=jnp.float32, precision=lax.Precision.HIGH
    )
    filtered = masked(
        multiply(left, right), lax.dynamic_slice_in_dim(keep, level * flags, flags, 1)
    )
    product = multiply(left, lax.all_gather(filtered, "row", axis=0, tiled=True))
    factor = DAMPING / (rows * lax.axis_size("row"))
    update = 1.5 * mine - 0.5 * factor * product
    return lax.all_to_all(update, "layer", split_axis=0, concat_axis=1, tiled=True)


def split(values):
    high = values.astype(jnp.bfloat16)
    low = (values - high.astype(jnp.float32)).astype(jnp.bfloat16)
    return high, low


def kernel(
    layers, block, factor,
    matrix, flags, out,
    raw, panel, a_high, a_low, both, total, staged, flags_in, flags_a, flags_x, flags_keep,
    send_sem, recv_sem, panel_send, panel_recv, flag_send, flag_recv, flag_local_sem, out_send, out_recv, local_sem,
):
    rows, cols = matrix.shape
    chunks = cols // layers // LANES
    tasks = 2 * chunks
    half = rows // 2
    share = rows // layers
    block_rows = rows // block
    row = lax.axis_index("row")
    col = lax.axis_index("col")
    level = lax.axis_index("layer")
    y, x = row // 2, row % 2
    along_x = {"row": y * 2 + (1 - x)}
    along_y = {"row": (1 - y) * 2 + x}
    across = {"row": (1 - y) * 2 + (1 - x)}
    twin = {"col": 1 - col}
    others = [{"layer": (level + step) % layers} for step in range(1, layers)]

    barrier = pltpu.get_barrier_semaphore()
    peers = [along_x, along_y, across, twin] + others
    for peer in peers:
        pl.semaphore_signal(barrier, inc=1, device_id=peer, device_id_type=MESH)
    pl.semaphore_wait(barrier, len(peers))

    def remote(source, target, sent, landed, peer):
        return pltpu.make_async_remote_copy(
            src_ref=source, dst_ref=target, send_sem=sent, recv_sem=landed,
            device_id=peer, device_id_type=MESH,
        )

    def part(task, slot, top):
        return raw.at[task, slot, pl.ds(top * half, half)]

    def move(task, arrival, source):
        slot, top = ((1, 0), (1, 1), (2, 1), (2, 0), (3, 0), (3, 1))[arrival]
        peer = along_x if arrival in (0, 1, 5) else along_y
        return remote(
            source, part(task, slot, top), send_sem.at[task, arrival], recv_sem.at[task, arrival], peer
        )

    def own_x(task, top):
        start = pl.multiple_of((level * chunks + task) * LANES, LANES)
        return matrix.at[pl.ds(top * half, half), pl.ds(start, LANES)]

    def send_x(task):
        for arrival, top in ((0, 0), (2, 1), (1, 1), (3, 0)):
            move(task, arrival, own_x(task, top)).start()

    def send_f(task):
        for arrival, top in ((0, 0), (2, 1), (1, 1), (3, 0)):
            move(task, arrival, part(task, 0, top)).start()

    def hand_on(task):
        move(task, 0, part(task, 1, 0)).wait_recv()
        move(task, 4, part(task, 1, 0)).start()
        move(task, 2, part(task, 2, 1)).wait_recv()
        move(task, 5, part(task, 2, 1)).start()

    @pl.when(col == 1)
    def _():
        send_x(0)

    flag_local = [
        pltpu.make_async_copy(flags.at[n], flags_in.at[4 + n], flag_local_sem.at[n]) for n in range(2)
    ]
    for copy in flag_local:
        copy.start()
    flag_moves = [
        remote(flags.at[0], flags_in.at[n], flag_send.at[n], flag_recv.at[n], peer)
        for n, peer in enumerate((along_x, along_y, across, twin))
    ]
    for copy in flag_moves:
        copy.start()
    bands = slices = 4
    tall = rows // bands

    def band(n):
        return pl.ds(n * tall, tall)

    panel_moves = [
        remote(matrix.at[band(n)], panel.at[band(n)], panel_send.at[n], panel_recv.at[n], twin)
        for n in range(bands)
    ]
    def own_panel(n):
        return raw.at[chunks + n // 4, n % 4]

    panel_local = [
        pltpu.make_async_copy(
            matrix.at[:, pl.ds(n * LANES, LANES)], own_panel(n), local_sem.at[2 * chunks + n]
        )
        for n in range(cols // LANES)
    ]
    piece_local = [
        pltpu.make_async_copy(
            matrix.at[:, pl.ds(pl.multiple_of((level * chunks + n) * LANES, LANES), LANES)],
            raw.at[n, 0],
            local_sem.at[n],
        )
        for n in range(chunks)
    ]
    for copy in panel_moves + panel_local + piece_local:
        copy.start()

    def expand(flags, first, width):
        index = lax.broadcasted_iota(jnp.int32, (flags.shape[1], width), 0)
        lane = lax.broadcasted_iota(jnp.int32, (flags.shape[1], width), 1)
        start = (index - first) * block
        table = jnp.where((lane >= start) & (lane < start + block), 1.0, 0.0)
        return jnp.dot(
            flags.astype(jnp.float32).astype(jnp.bfloat16), table.astype(jnp.bfloat16), preferred_element_type=jnp.float32
        )

    per_chunk = LANES // block

    def expand_chunks(flags, store):
        for n in range(chunks):
            store(n, expand(flags, (level * chunks + n) * per_chunk, LANES))

    def store_x(slot):
        def store(n, values):
            flags_x[n, slot] = values
        return store

    def store_keep(n, values):
        flags_keep[n] = values

    group = 8

    def prepare_panel(side, owner_col):
        for n in range(cols // half):
            owner = owner_col * (cols // rows) + n // 2
            slot = (owner // 2 + y) % 2 * 2 + (owner % 2 + x) % 2
            place = slot * 2 + n % 2

            def body(i, carry):
                base = pl.multiple_of(i * group, group)
                for m in range(half // LANES):
                    lanes = n * half + m * LANES
                    flags = flags_a[side, pl.ds(base, group), lanes : lanes + LANES]
                    for b in range(group):
                        at = pl.ds(pl.multiple_of((i * group + b) * block, block), block)
                        if side:
                            values = panel[at, lanes : lanes + LANES]
                        else:
                            values = own_panel(lanes // LANES)[at, :]
                        high, low = split(values * flags[b : b + 1])
                        a_high[place, at, m * LANES : (m + 1) * LANES] = high
                        a_low[place, at, m * LANES : (m + 1) * LANES] = low
                return carry

            lax.fori_loop(0, block_rows // group, body, 0)

    def at_block(i, b):
        return pl.ds(pl.multiple_of((i * group + b) * block, block), block)

    def convert(task, slot, top):
        which = task - (task // chunks) * (task - chunks)

        def body(i, carry):
            flags = flags_x[which, slot, pl.ds(pl.multiple_of(i * group, group), group), :]
            for b in range(group):
                at = at_block(i, b)
                high, low = split(raw[task, slot, at, :] * flags[b : b + 1])
                both[at, 0:LANES] = high
                both[at, LANES : 2 * LANES] = low
            return carry

        steps = block_rows // group // 2
        lax.fori_loop(top * steps, (top + 1) * steps, body, 0)

    def out_move(n, step):
        target = (level + step) % layers
        start = pl.multiple_of((level * chunks + n) * LANES, LANES)
        return remote(
            staged.at[n, pl.ds(pl.multiple_of(target * share, share), share)],
            out.at[:, pl.ds(start, LANES)],
            out_send.at[n, step - 1],
            out_recv.at[n, step - 1],
            {"layer": target},
        )

    def out_local(n):
        start = pl.multiple_of((level * chunks + n) * LANES, LANES)
        return pltpu.make_async_copy(
            staged.at[n, pl.ds(pl.multiple_of(level * share, share), share)],
            out.at[:, pl.ds(start, LANES)],
            local_sem.at[chunks + n],
        )

    def finish_rows(task, tile):
        steps = block_rows // group // slices

        def square(i, carry):
            flags = flags_keep[task, pl.ds(pl.multiple_of(i * group, group), group), :]
            for b in range(group):
                at = at_block(i, b)
                summed = total[at, 0:LANES] + total[at, LANES : 2 * LANES]
                raw[task + chunks, 0, at, :] = summed * flags[b : b + 1]
            return carry

        def update(i, carry):
            n = task - chunks
            flags = flags_x[n, 0, pl.ds(pl.multiple_of(i * group, group), group), :]
            for b in range(group):
                at = at_block(i, b)
                summed = total[at, 0:LANES] + total[at, LANES : 2 * LANES]
                staged[n, at, :] = 1.5 * (raw[n, 0, at, :] * flags[b : b + 1]) - factor * summed
            return carry

        @pl.when(task < chunks)
        def _():
            lax.fori_loop(tile * steps, (tile + 1) * steps, square, 0)

        @pl.when(task >= chunks)
        def _():
            lax.fori_loop(tile * steps, (tile + 1) * steps, update, 0)

    def finish(task):
        total[...] = jnp.zeros_like(total)
        first_tile = 1 - level * 2 // layers

        def pair(g, carry):
            other = g % 2 * 2 + g // 2

            @pl.when(g >= 2)
            def _():
                for slot, top, arrival in ((g, 0, g + 1), (other, 1, 4 * g - 7)):
                    remote(
                        part(task, slot, top), part(task, slot, top),
                        send_sem.at[task, arrival], recv_sem.at[task, arrival], along_x,
                    ).wait_recv()

            convert(task, g, 0)
            convert(task, other, 1)

            def multiply(i, carry):
                tile = (first_tile * (slices // 2) + i) % slices
                at = pl.ds(pl.multiple_of(tile * tall, tall), tall)
                value = total[at, :]
                for place, rows_of in ((g * 2, both.at[0:half]), (other * 2 + 1, both.at[half:rows])):
                    for side in (a_high, a_low):
                        value += jnp.dot(
                            side[place, at, :], rows_of[...], preferred_element_type=jnp.float32
                        )
                total[at, :] = value

                @pl.when(g == 3)
                def _():
                    finish_rows(task, tile)

                for step in range(1, layers):
                    target = (level + step) % layers

                    @pl.when((g == 3) & (task >= chunks) & (target * slices // layers == tile))
                    def _():
                        out_move(task - chunks, step).start()

                return carry

            lax.fori_loop(0, slices, multiply, 0)
            return carry

        lax.fori_loop(0, 4, pair, 0)

        @pl.when(task >= chunks)
        def _():
            out_local(task - chunks).start()

    def prepare_own():
        for copy in panel_local:
            copy.wait()
        prepare_panel(0, col)

    def send(task):
        @pl.when(task < chunks)
        def _():
            send_x(task)

        @pl.when((task >= chunks) & (task < tasks))
        def _():
            send_f(task)

    for copy in flag_local:
        copy.wait()
    flags_a[0] = expand(flags_in[4], 0, cols)

    @pl.when(col == 1)
    def _():
        hand_on(0)
        send_x(1)

    prepare_own()

    @pl.when(col == 0)
    def _():
        send_x(0)

    expand_chunks(flags_in[4], store_x(0))
    expand_chunks(flags_in[5], store_keep)
    flags_x[chunks] = jnp.ones_like(flags_x[chunks])
    for copy in piece_local:
        copy.wait()

    @pl.when(col == 0)
    def _():
        hand_on(0)
        send_x(1)

    for copy in flag_moves:
        copy.wait_recv()
    flags_a[1] = expand(flags_in[3], 0, cols)
    for slot in (1, 2, 3):
        expand_chunks(flags_in[slot - 1], store_x(slot))
    for copy in panel_moves:
        copy.wait_recv()
    prepare_panel(1, 1 - col)
    finish(0)

    def advance(task, carry):
        hand_on(task)
        send(task + 1)
        finish(task)
        return carry

    lax.fori_loop(1, tasks, advance, 0)

    for copy in flag_moves + panel_moves:
        copy.wait_send()

    def drain(task, carry):
        for arrival in range(6):
            move(task, arrival, part(task, 0, 0)).wait_send()
        return carry

    lax.fori_loop(0, tasks, drain, 0)

    def drain_out(n, carry):
        for step in range(1, layers):
            out_move(n, step).wait()
        out_local(n).wait()
        return carry

    lax.fori_loop(0, chunks, drain_out, 0)


def fused(matrix, pattern, keep):
    rows, cols = matrix.shape
    layers = lax.axis_size("layer")
    block_rows, block_cols = pattern.shape
    block = rows // block_rows
    chunks = cols // layers // LANES
    tasks = 2 * chunks
    half = rows // 2
    factor = 0.5 * DAMPING / (rows * lax.axis_size("row"))

    vmem = pl.BlockSpec(memory_space=pltpu.VMEM)
    anywhere = pl.BlockSpec(memory_space=pl.ANY)
    dma = pltpu.SemaphoreType.DMA
    return pl.pallas_call(
        functools.partial(kernel, layers, block, factor),
        out_shape=jax.ShapeDtypeStruct((rows // layers, cols), jnp.float32),
        in_specs=[anywhere, anywhere],
        out_specs=vmem,
        scratch_shapes=[
            pltpu.VMEM((tasks, 4, rows, LANES), jnp.float32),
            pltpu.VMEM((rows, cols), jnp.float32),
            pltpu.VMEM((8, rows, half), jnp.bfloat16),
            pltpu.VMEM((8, rows, half), jnp.bfloat16),
            pltpu.VMEM((rows, 2 * LANES), jnp.bfloat16),
            pltpu.VMEM((rows, 2 * LANES), jnp.float32),
            pltpu.VMEM((chunks, rows, LANES), jnp.float32),
            pltpu.VMEM((6, block_rows, block_cols), jnp.int32),
            pltpu.VMEM((2, block_rows, cols), jnp.float32),
            pltpu.VMEM((chunks + 1, 4, block_rows, LANES), jnp.float32),
            pltpu.VMEM((chunks, block_rows, LANES), jnp.float32),
            dma((tasks, 6)),
            dma((tasks, 6)),
            dma((4,)),
            dma((4,)),
            dma((4,)),
            dma((4,)),
            dma((2,)),
            dma((chunks, max(layers - 1, 1))),
            dma((chunks, max(layers - 1, 1))),
            dma((2 * chunks + cols // LANES,)),
        ],
        compiler_params=pltpu.CompilerParams(
            collective_id=0, has_side_effects=True, vmem_limit_bytes=52_000_000
        ),
    )(matrix, jnp.stack([pattern, keep]))


def local(matrix, pattern, keep):
    rows, cols = matrix.shape
    layers = lax.axis_size("layer")
    block = rows // pattern.shape[0]
    fits = (
        lax.axis_size("row") == 4
        and lax.axis_size("col") == 2
        and cols % (layers * LANES) == 0
        and cols // (layers * LANES) >= 3
        and LANES % block == 0
        and block % 16 == 0
        and rows % (16 * block) == 0
        and rows % (8 * layers) == 0
        and (rows // 2) % LANES == 0
        and rows * cols <= 1 << 21
        and layers in (1, 2, 4)
    )
    return (fused if fits else plain)(matrix, pattern, keep)


def solution(mesh):
    placed = (P("row", "col"), P("row", "col"), P("row", "col"))
    return jax.shard_map(
        local, mesh=mesh, in_specs=placed, out_specs=P(("row", "layer"), "col"), check_vma=False
    )
```

```python
import functools

import jax
import jax.numpy as jnp
from jax import lax
from jax.experimental import pallas as pl
from jax.experimental.pallas import tpu as pltpu
from jax.sharding import PartitionSpec as P

MESH = pl.DeviceIdType.MESH
LANES = 128
DAMPING = 0.72


def masked(values, flags):
    rows, cols = values.shape
    block_rows, block_cols = flags.shape
    shaped = values.reshape(block_rows, rows // block_rows, block_cols, cols // block_cols)
    return (shaped * flags.astype(jnp.float32)[:, None, :, None]).reshape(rows, cols)


def plain(matrix, pattern, keep):
    rows, cols = matrix.shape
    layers = lax.axis_size("layer")
    level = lax.axis_index("layer")
    width = cols // layers
    flags = pattern.shape[1] // layers
    sparse = masked(matrix, pattern)
    left = lax.all_gather(sparse, "col", axis=1, tiled=True)
    mine = lax.dynamic_slice_in_dim(sparse, level * width, width, 1)
    right = lax.all_gather(mine, "row", axis=0, tiled=True)
    multiply = functools.partial(
        jnp.dot, preferred_element_type=jnp.float32, precision=lax.Precision.HIGH
    )
    filtered = masked(
        multiply(left, right), lax.dynamic_slice_in_dim(keep, level * flags, flags, 1)
    )
    product = multiply(left, lax.all_gather(filtered, "row", axis=0, tiled=True))
    factor = DAMPING / (rows * lax.axis_size("row"))
    update = 1.5 * mine - 0.5 * factor * product
    return lax.all_to_all(update, "layer", split_axis=0, concat_axis=1, tiled=True)


def split(values):
    high = values.astype(jnp.bfloat16)
    low = (values - high.astype(jnp.float32)).astype(jnp.bfloat16)
    return high, low


def kernel(
    layers, block, factor,
    matrix, flags, out,
    raw, panel, a_high, a_low, both, total, flags_in, flags_a, flags_x, flags_keep,
    lent, lent_high, lent_low, flags_far, flags_lent_keep,
    send_sem, recv_sem, panel_send, panel_recv, flag_send, flag_recv, flag_local_sem, out_send, out_recv, local_sem,
    lent_send, lent_recv, lent_local, twin_sem, far_sem,
):
    rows, cols = matrix.shape
    chunks = cols // layers // LANES
    tasks = 2 * chunks
    half = rows // 2
    share = rows // layers
    extra = rows // 8
    block_rows = rows // block
    row = lax.axis_index("row")
    col = lax.axis_index("col")
    level = lax.axis_index("layer")
    y, x = row // 2, row % 2
    along_x = {"row": y * 2 + (1 - x)}
    along_y = {"row": (1 - y) * 2 + x}
    across = {"row": (1 - y) * 2 + (1 - x)}
    twin = {"col": 1 - col}
    others = [{"layer": (level + step) % layers} for step in range(1, layers)]

    barrier = pltpu.get_barrier_semaphore()
    peers = [along_x, along_y, across, twin] + others
    for peer in peers:
        pl.semaphore_signal(barrier, inc=1, device_id=peer, device_id_type=MESH)
    pl.semaphore_wait(barrier, len(peers))

    def remote(source, target, sent, landed, peer):
        return pltpu.make_async_remote_copy(
            src_ref=source, dst_ref=target, send_sem=sent, recv_sem=landed,
            device_id=peer, device_id_type=MESH,
        )

    def part(task, slot, top):
        return raw.at[task, slot, pl.ds(top * half, half)]

    def move(task, arrival, source):
        slot, first, count = (
            (1, extra, half - extra), (1, half, half), (2, half, half - extra), (2, 0, half),
            (3, 0, half), (3, half, half), (1, 0, extra), (2, rows - extra, extra),
        )[arrival]
        peer = along_x if arrival in (0, 1, 5, 6) else along_y
        return remote(
            source(first, count), raw.at[task, slot, pl.ds(first, count)],
            send_sem.at[task, arrival], recv_sem.at[task, arrival], peer,
        )

    def own_x(task):
        start = pl.multiple_of((level * chunks + task) * LANES, LANES)
        return lambda first, count: matrix.at[pl.ds(first, count), pl.ds(start, LANES)]

    def in_slot(task, slot):
        return lambda first, count: raw.at[task, slot, pl.ds(first, count)]

    def send_first():
        for task in range(chunks):
            for arrival in (6, 7):
                move(task, arrival, own_x(task)).start()

    def send_x(task):
        for arrival in (0, 2, 1, 3):
            move(task, arrival, own_x(task)).start()

    def send_f(task):
        for arrival in (0, 2, 1, 3):
            move(task, arrival, in_slot(task, 0)).start()

    def hand_on(task):
        move(task, 0, in_slot(task, 1)).wait_recv()
        move(task, 4, in_slot(task, 1)).start()
        move(task, 2, in_slot(task, 2)).wait_recv()
        move(task, 5, in_slot(task, 2)).start()

    def lent_rows(k):
        return raw.at[pl.ds(0, chunks), 1 + k, pl.ds(k * (rows - extra), extra)]

    def lent_slot(source, k):
        return lent.at[pl.ds(source * chunks, chunks), pl.ds(k * extra, extra)]

    def lend(k, step, source):
        return remote(
            lent_rows(k), lent_slot(source, k), lent_send.at[k, step - 1], lent_recv.at[k, step - 1],
            {"layer": (level + step) % layers},
        )

    def lend_here(k):
        return pltpu.make_async_copy(lent_rows(k), lent_slot(level, k), lent_local.at[k])

    from_twin = panel.at[:, pl.ds(2 * extra, 2 * extra)]
    lend_twin = remote(lent, from_twin, twin_sem.at[0], twin_sem.at[1], twin)

    def lend_all():
        for task in range(chunks):
            for arrival in (6, 7):
                move(task, arrival, in_slot(task, 1)).wait_recv()
        for k in range(2):
            for step in range(1, layers):
                lend(k, step, level).start()
            lend_here(k).start()

    def pass_lent():
        for k in range(2):
            for step in range(1, layers):
                lend(k, step, (level + layers - step) % layers).wait_recv()
            lend_here(k).wait()
        lend_twin.start()

    send_first()

    @pl.when(col == 1)
    def _():
        send_x(0)

    flag_local = [
        pltpu.make_async_copy(flags.at[n], flags_in.at[4 + n], flag_local_sem.at[n]) for n in range(2)
    ]
    for copy in flag_local:
        copy.start()
    flag_moves = [
        remote(flags.at[0], flags_in.at[n], flag_send.at[n], flag_recv.at[n], peer)
        for n, peer in enumerate((along_x, along_y, across, twin))
    ] + [
        remote(flags.at[1], flags_in.at[6 + n], flag_send.at[4 + n], flag_recv.at[4 + n], peer)
        for n, peer in enumerate((along_x, along_y))
    ]
    flags_on = remote(flags_in.at[pl.ds(0, 2)], flags_far, far_sem.at[0], far_sem.at[1], twin)
    for copy in flag_moves:
        copy.start()
    slices = 4
    tall = rows // slices

    panel_moves = [
        remote(
            matrix.at[:, pl.ds(n * LANES, LANES)], panel.at[n], panel_send.at[n], panel_recv.at[n], twin
        )
        for n in range(cols // LANES)
    ]
    def own_panel(n):
        return raw.at[chunks + n // 4, n % 4]

    panel_local = [
        pltpu.make_async_copy(
            matrix.at[:, pl.ds(n * LANES, LANES)], own_panel(n), local_sem.at[2 * chunks + n]
        )
        for n in range(cols // LANES)
    ]
    piece_local = [
        pltpu.make_async_copy(
            matrix.at[:, pl.ds(pl.multiple_of((level * chunks + n) * LANES, LANES), LANES)],
            raw.at[n, 0],
            local_sem.at[n],
        )
        for n in range(chunks)
    ]
    for copy in panel_moves + panel_local + piece_local:
        copy.start()

    def expand(flags, first, width):
        index = lax.broadcasted_iota(jnp.int32, (flags.shape[1], width), 0)
        lane = lax.broadcasted_iota(jnp.int32, (flags.shape[1], width), 1)
        start = (index - first) * block
        table = jnp.where((lane >= start) & (lane < start + block), 1.0, 0.0)
        return jnp.dot(
            flags.astype(jnp.float32).astype(jnp.bfloat16), table.astype(jnp.bfloat16), preferred_element_type=jnp.float32
        )

    per_chunk = LANES // block

    def expand_chunks(flags, store):
        for n in range(chunks):
            store(n, expand(flags, (level * chunks + n) * per_chunk, LANES))

    def store_x(slot):
        def store(n, values):
            flags_x[n, slot] = values
        return store

    def store_lent(k):
        def store(n, values):
            flags_lent_keep[n, k] = values
        return store

    def store_keep(n, values):
        flags_keep[n] = values

    group = 8

    def prepare_panel(side, owner_col):
        for n in range(cols // half):
            owner = owner_col * (cols // rows) + n // 2
            slot = (owner // 2 + y) % 2 * 2 + (owner % 2 + x) % 2
            place = slot * 2 + n % 2

            def body(i, carry):
                base = pl.multiple_of(i * group, group)
                for m in range(half // LANES):
                    lanes = n * half + m * LANES
                    flags = flags_a[side, pl.ds(base, group), lanes : lanes + LANES]
                    for b in range(group):
                        at = pl.ds(pl.multiple_of((i * group + b) * block, block), block)
                        if side:
                            values = panel[lanes // LANES, at, :]
                        else:
                            values = own_panel(lanes // LANES)[at, :]
                        high, low = split(values * flags[b : b + 1])
                        a_high[place, at, m * LANES : (m + 1) * LANES] = high
                        a_low[place, at, m * LANES : (m + 1) * LANES] = low
                return carry

            lax.fori_loop(0, block_rows // group, body, 0)

    def at_block(i, b):
        return pl.ds(pl.multiple_of((i * group + b) * block, block), block)

    def convert(task, slot, top):
        which = task - (task // chunks) * (task - chunks)

        def body(i, carry):
            flags = flags_x[which, slot, pl.ds(pl.multiple_of(i * group, group), group), :]
            for b in range(group):
                at = at_block(i, b)
                high, low = split(raw[task, slot, at, :] * flags[b : b + 1])
                both[at, 0:LANES] = high
                both[at, LANES : 2 * LANES] = low
            return carry

        steps = block_rows // group // 2
        lax.fori_loop(top * steps, (top + 1) * steps, body, 0)

    def staged(n):
        return raw.at[n, 3]

    def out_move(n, step):
        target = (level + step) % layers
        start = pl.multiple_of((level * chunks + n) * LANES, LANES)
        return remote(
            staged(n).at[pl.ds(pl.multiple_of(target * share, share), share)],
            out.at[:, pl.ds(start, LANES)],
            out_send.at[n, step - 1],
            out_recv.at[n, step - 1],
            {"layer": target},
        )

    def out_local(n):
        start = pl.multiple_of((level * chunks + n) * LANES, LANES)
        return pltpu.make_async_copy(
            staged(n).at[pl.ds(pl.multiple_of(level * share, share), share)],
            out.at[:, pl.ds(start, LANES)],
            local_sem.at[chunks + n],
        )

    def finish_rows(task, second, tile):
        steps = block_rows // group // slices

        def square(i, carry):
            flags = flags_keep[task, pl.ds(pl.multiple_of(i * group, group), group), :]
            for b in range(group):
                at = at_block(i, b)
                summed = total[at, 0:LANES] + total[at, LANES : 2 * LANES]
                raw[task + chunks, 0, at, :] = summed * flags[b : b + 1]
            return carry

        def update(i, carry):
            n = task - chunks
            flags = flags_x[n, 0, pl.ds(pl.multiple_of(i * group, group), group), :]
            for b in range(group):
                at = at_block(i, b)
                summed = total[at, 0:LANES] + total[at, LANES : 2 * LANES]
                raw[n, 3, at, :] = 1.5 * (raw[n, 0, at, :] * flags[b : b + 1]) - factor * summed
            return carry

        lax.fori_loop(tile * steps, (tile + 1) * steps, update if second else square, 0)

    def finish(task, second):
        total[...] = jnp.zeros_like(total)
        first_tile = 1 - level * 2 // layers

        def pair(g, carry):
            other = g % 2 * 2 + g // 2

            @pl.when(g >= 2)
            def _():
                for slot, top, arrival in ((g, 0, g + 1), (other, 1, 4 * g - 7)):
                    remote(
                        part(task, slot, top), part(task, slot, top),
                        send_sem.at[task, arrival], recv_sem.at[task, arrival], along_x,
                    ).wait_recv()

            convert(task, g, 0)
            convert(task, other, 1)

            def multiply(i, carry):
                tile = (first_tile * (slices // 2) + i) % slices
                at = pl.ds(pl.multiple_of(tile * tall, tall), tall)
                value = total[at, :]
                for place, rows_of in ((g * 2, both.at[0:half]), (other * 2 + 1, both.at[half:rows])):
                    for side in (a_high, a_low):
                        value += jnp.dot(
                            side[place, at, :], rows_of[...], preferred_element_type=jnp.float32
                        )
                total[at, :] = value

                @pl.when(g == 3)
                def _():
                    finish_rows(task, second, tile)

                for step in range(1, layers if second else 1):
                    target = (level + step) % layers

                    @pl.when((g == 3) & (target * slices // layers == tile))
                    def _():
                        out_move(task - chunks, step).start()

                return carry

            lax.fori_loop(0, slices, multiply, 0)
            return carry

        lax.fori_loop(0, 4, pair, 0)

        if second:
            out_local(task - chunks).start()

    def prepare_lent():
        for side, owner_col in ((0, col), (1, 1 - col)):
            for n in range(cols // LANES):
                owner = owner_col * (cols // rows) + n * LANES // rows
                slot = (owner // 2 + y) % 2 * 2 + (owner % 2 + x) % 2
                place = slot * 2 + n * LANES // half % 2
                lanes = n * LANES % half
                for k in range(2):
                    for b in range(extra // block):
                        flag = (side * 2 + k) * block_rows + k * (block_rows - extra // block) + b
                        at = slice(k * extra + b * block, k * extra + (b + 1) * block)
                        values = from_twin[n, at, :] if side else lent[n, at, :]
                        values = values * panel[n, flag : flag + 1, :]
                        high, low = split(values)
                        lent_high[place, at, lanes : lanes + LANES] = high
                        lent_low[place, at, lanes : lanes + LANES] = low

    def square_lent(n):
        total[0 : 2 * extra, :] = jnp.zeros((2 * extra, 2 * LANES), jnp.float32)

        def pair(g, carry):
            other = g % 2 * 2 + g // 2
            convert(n, g, 0)
            convert(n, other, 1)
            value = total[0 : 2 * extra, :]
            for place, rows_of in ((g * 2, both.at[0:half]), (other * 2 + 1, both.at[half:rows])):
                for side in (lent_high, lent_low):
                    value += jnp.dot(side[place], rows_of[...], preferred_element_type=jnp.float32)
            total[0 : 2 * extra, :] = value
            return carry

        lax.fori_loop(0, 4, pair, 0)
        for k in range(2):
            for b in range(extra // block):
                flag = k * (block_rows - extra // block) + b
                at = slice(k * extra + b * block, k * extra + (b + 1) * block)
                to = k * (rows - extra) + b * block
                summed = total[at, 0:LANES] + total[at, LANES : 2 * LANES]
                raw[n + chunks, 1 + k, to : to + block, :] = summed * flags_lent_keep[n, k, flag : flag + 1, :]

    def prepare_own():
        for copy in panel_local:
            copy.wait()
        prepare_panel(0, col)

    for copy in flag_local:
        copy.wait()
    flags_a[0] = expand(flags_in[4], 0, cols)

    @pl.when(col == 1)
    def _():
        lend_all()
        hand_on(0)
        send_x(1)

    prepare_own()

    @pl.when(col == 0)
    def _():
        lend_all()
        send_x(0)

    expand_chunks(flags_in[4], store_x(0))
    expand_chunks(flags_in[5], store_keep)
    flags_x[chunks] = jnp.ones_like(flags_x[chunks])
    for copy in piece_local:
        copy.wait()

    @pl.when(col == 0)
    def _():
        hand_on(0)
        send_x(1)

    for copy in flag_moves:
        copy.wait_recv()
    flags_a[1] = expand(flags_in[3], 0, cols)
    for slot in (1, 2, 3):
        expand_chunks(flags_in[slot - 1], store_x(slot))
    for copy in panel_moves:
        copy.wait_recv()
    prepare_panel(1, 1 - col)
    flags_on.start()
    flags_on.wait_recv()
    for k in range(2):
        for side, source in ((0, flags_in), (1, flags_far)):
            values = expand(source[k], 0, cols)
            first_row = (side * 2 + k) * block_rows
            for n in range(cols // LANES):
                panel[n, first_row : first_row + block_rows, :] = values[:, n * LANES : (n + 1) * LANES]
        expand_chunks(flags_in[6 + k], store_lent(k))
    finish(0, False)

    def first(task, carry):
        hand_on(task)

        @pl.when(task + 1 < chunks)
        def _():
            send_x(task + 1)

        @pl.when(task + 1 == chunks)
        def _():
            send_f(chunks)

        @pl.when(task + 1 == chunks)
        def _():
            pass_lent()

        finish(task, False)
        return carry

    lax.fori_loop(1, chunks, first, 0)
    lend_twin.wait_recv()
    prepare_lent()
    square_lent(0)

    def second(task, carry):
        hand_on(task)

        @pl.when(task + 1 < tasks)
        def _():
            send_f(task + 1)
            square_lent(task + 1 - chunks)

        finish(task, True)
        return carry

    lax.fori_loop(chunks, tasks, second, 0)
    flags_on.wait_send()

    for copy in flag_moves + panel_moves:
        copy.wait_send()

    def drain(n, carry):
        for arrival in range(8):
            move(n, arrival, in_slot(n, 0)).wait_send()
        for arrival in range(6):
            move(n + chunks, arrival, in_slot(n, 0)).wait_send()
        return carry

    lax.fori_loop(0, chunks, drain, 0)
    for k in range(2):
        for step in range(1, layers):
            lend(k, step, level).wait_send()
    lend_twin.wait_send()

    def drain_out(n, carry):
        for step in range(1, layers):
            out_move(n, step).wait()
        out_local(n).wait()
        return carry

    lax.fori_loop(0, chunks, drain_out, 0)


def fused(matrix, pattern, keep):
    rows, cols = matrix.shape
    layers = lax.axis_size("layer")
    block_rows, block_cols = pattern.shape
    block = rows // block_rows
    chunks = cols // layers // LANES
    tasks = 2 * chunks
    half = rows // 2
    factor = 0.5 * DAMPING / (rows * lax.axis_size("row"))

    vmem = pl.BlockSpec(memory_space=pltpu.VMEM)
    anywhere = pl.BlockSpec(memory_space=pl.ANY)
    dma = pltpu.SemaphoreType.DMA
    return pl.pallas_call(
        functools.partial(kernel, layers, block, factor),
        out_shape=jax.ShapeDtypeStruct((rows // layers, cols), jnp.float32),
        in_specs=[anywhere, anywhere],
        out_specs=vmem,
        scratch_shapes=[
            pltpu.VMEM((tasks, 4, rows, LANES), jnp.float32),
            pltpu.VMEM((cols // LANES, rows, LANES), jnp.float32),
            pltpu.VMEM((8, rows, half), jnp.bfloat16),
            pltpu.VMEM((8, rows, half), jnp.bfloat16),
            pltpu.VMEM((rows, 2 * LANES), jnp.bfloat16),
            pltpu.VMEM((rows, 2 * LANES), jnp.float32),
            pltpu.VMEM((8, block_rows, block_cols), jnp.int32),
            pltpu.VMEM((2, block_rows, cols), jnp.float32),
            pltpu.VMEM((chunks + 1, 4, block_rows, LANES), jnp.float32),
            pltpu.VMEM((chunks, block_rows, LANES), jnp.float32),
            pltpu.VMEM((cols // LANES, rows // 4, LANES), jnp.float32),
            pltpu.VMEM((8, rows // 4, half), jnp.bfloat16),
            pltpu.VMEM((8, rows // 4, half), jnp.bfloat16),
            pltpu.VMEM((2, block_rows, block_cols), jnp.int32),
            pltpu.VMEM((chunks, 2, block_rows, LANES), jnp.float32),
            dma((tasks, 8)),
            dma((tasks, 8)),
            dma((cols // LANES,)),
            dma((cols // LANES,)),
            dma((6,)),
            dma((6,)),
            dma((2,)),
            dma((chunks, max(layers - 1, 1))),
            dma((chunks, max(layers - 1, 1))),
            dma((2 * chunks + cols // LANES,)),
            dma((2, max(layers - 1, 1))),
            dma((2, max(layers - 1, 1))),
            dma((2,)),
            dma((2,)),
            dma((2,)),
        ],
        compiler_params=pltpu.CompilerParams(
            collective_id=0, has_side_effects=True, vmem_limit_bytes=54_200_000
        ),
    )(matrix, jnp.stack([pattern, keep]))


def local(matrix, pattern, keep):
    rows, cols = matrix.shape
    layers = lax.axis_size("layer")
    block = rows // pattern.shape[0]
    fits = (
        lax.axis_size("row") == 4
        and lax.axis_size("col") == 2
        and cols % (layers * LANES) == 0
        and cols // (layers * LANES) >= 3
        and LANES % block == 0
        and block % 16 == 0
        and rows % (32 * block) == 0
        and rows % (8 * layers) == 0
        and (rows // 2) % LANES == 0
        and rows * cols <= 1 << 21
        and layers in (1, 2, 4)
    )
    return (fused if fits else plain)(matrix, pattern, keep)


def solution(mesh):
    placed = (P("row", "col"), P("row", "col"), P("row", "col"))
    return jax.shard_map(
        local, mesh=mesh, in_specs=placed, out_specs=P(("row", "layer"), "col"), check_vma=False
    )
```

```python
import functools

import jax
import jax.numpy as jnp
from jax import lax
from jax.experimental import pallas as pl
from jax.experimental.pallas import tpu as pltpu
from jax.sharding import PartitionSpec as P

MESH = pl.DeviceIdType.MESH
LANES = 128
DAMPING = 0.72


def masked(values, flags):
    rows, cols = values.shape
    block_rows, block_cols = flags.shape
    shaped = values.reshape(block_rows, rows // block_rows, block_cols, cols // block_cols)
    return (shaped * flags.astype(jnp.float32)[:, None, :, None]).reshape(rows, cols)


def plain(matrix, pattern, keep):
    rows, cols = matrix.shape
    layers = lax.axis_size("layer")
    level = lax.axis_index("layer")
    width = cols // layers
    flags = pattern.shape[1] // layers
    sparse = masked(matrix, pattern)
    left = lax.all_gather(sparse, "col", axis=1, tiled=True)
    mine = lax.dynamic_slice_in_dim(sparse, level * width, width, 1)
    right = lax.all_gather(mine, "row", axis=0, tiled=True)
    multiply = functools.partial(
        jnp.dot, preferred_element_type=jnp.float32, precision=lax.Precision.HIGH
    )
    filtered = masked(
        multiply(left, right), lax.dynamic_slice_in_dim(keep, level * flags, flags, 1)
    )
    product = multiply(left, lax.all_gather(filtered, "row", axis=0, tiled=True))
    factor = DAMPING / (rows * lax.axis_size("row"))
    update = 1.5 * mine - 0.5 * factor * product
    return lax.all_to_all(update, "layer", split_axis=0, concat_axis=1, tiled=True)


def split(values):
    high = values.astype(jnp.bfloat16)
    low = (values - high.astype(jnp.float32)).astype(jnp.bfloat16)
    return high, low


def kernel(
    layers, block, factor,
    matrix, flags, out,
    raw, panel, a_high, a_low, both, total, flags_in, flags_a, flags_x, flags_keep,
    lent, lent_high, lent_low, flags_far, flags_lent_keep,
    send_sem, recv_sem, panel_send, panel_recv, flag_send, flag_recv, flag_local_sem, out_send, out_recv, local_sem,
    lent_send, lent_recv, lent_local, twin_sem, far_sem,
):
    rows, cols = matrix.shape
    chunks = cols // layers // LANES
    tasks = 2 * chunks
    half = rows // 2
    share = rows // layers
    extra = rows // 8
    block_rows = rows // block
    row = lax.axis_index("row")
    col = lax.axis_index("col")
    level = lax.axis_index("layer")
    y, x = row // 2, row % 2
    along_x = {"row": y * 2 + (1 - x)}
    along_y = {"row": (1 - y) * 2 + x}
    across = {"row": (1 - y) * 2 + (1 - x)}
    twin = {"col": 1 - col}
    others = [{"layer": (level + step) % layers} for step in range(1, layers)]

    barrier = pltpu.get_barrier_semaphore()
    peers = [along_x, along_y, across, twin] + others
    for peer in peers:
        pl.semaphore_signal(barrier, inc=1, device_id=peer, device_id_type=MESH)
    pl.semaphore_wait(barrier, len(peers))

    def remote(source, target, sent, landed, peer):
        return pltpu.make_async_remote_copy(
            src_ref=source, dst_ref=target, send_sem=sent, recv_sem=landed,
            device_id=peer, device_id_type=MESH,
        )

    def part(task, slot, top):
        return raw.at[task, slot, pl.ds(top * half, half)]

    def move(task, arrival, source):
        slot, first, count = (
            (1, extra, half - extra), (1, half, half), (2, half, half - extra), (2, 0, half),
            (3, 0, half), (3, half, half), (1, 0, extra), (2, rows - extra, extra),
        )[arrival]
        peer = along_x if arrival in (0, 1, 5, 6) else along_y
        return remote(
            source(first, count), raw.at[task, slot, pl.ds(first, count)],
            send_sem.at[task, arrival], recv_sem.at[task, arrival], peer,
        )

    def own_x(task):
        start = pl.multiple_of((level * chunks + task) * LANES, LANES)
        return lambda first, count: matrix.at[pl.ds(first, count), pl.ds(start, LANES)]

    def in_slot(task, slot):
        return lambda first, count: raw.at[task, slot, pl.ds(first, count)]

    def send_first():
        for task in range(chunks):
            for arrival in (6, 7):
                move(task, arrival, own_x(task)).start()

    def send_x(task):
        for arrival in (0, 2, 1, 3):
            move(task, arrival, own_x(task)).start()

    def send_f(task):
        for arrival in (0, 2, 1, 3):
            move(task, arrival, in_slot(task, 0)).start()

    def hand_on(task):
        move(task, 0, in_slot(task, 1)).wait_recv()
        move(task, 4, in_slot(task, 1)).start()
        move(task, 2, in_slot(task, 2)).wait_recv()
        move(task, 5, in_slot(task, 2)).start()

    def lent_rows(k):
        return raw.at[pl.ds(0, chunks), 1 + k, pl.ds(k * (rows - extra), extra)]

    def lent_slot(source, k):
        return lent.at[pl.ds(source * chunks, chunks), pl.ds(k * extra, extra)]

    def lend(k, step, source):
        return remote(
            lent_rows(k), lent_slot(source, k), lent_send.at[k, step - 1], lent_recv.at[k, step - 1],
            {"layer": (level + step) % layers},
        )

    def lend_here(k):
        return pltpu.make_async_copy(lent_rows(k), lent_slot(level, k), lent_local.at[k])

    from_twin = panel.at[:, pl.ds(2 * extra, 2 * extra)]
    lend_twin = remote(lent, from_twin, twin_sem.at[0], twin_sem.at[1], twin)

    def lend_all():
        for task in range(chunks):
            for arrival in (6, 7):
                move(task, arrival, in_slot(task, 1)).wait_recv()
        for k in range(2):
            for step in range(1, layers):
                lend(k, step, level).start()
            lend_here(k).start()

    def pass_lent():
        for k in range(2):
            for step in range(1, layers):
                lend(k, step, (level + layers - step) % layers).wait_recv()
            lend_here(k).wait()
        lend_twin.start()

    send_first()

    @pl.when(col == 1)
    def _():
        send_x(0)

    flag_local = [
        pltpu.make_async_copy(flags.at[n], flags_in.at[4 + n], flag_local_sem.at[n]) for n in range(2)
    ]
    for copy in flag_local:
        copy.start()
    flag_moves = [
        remote(flags.at[0], flags_in.at[n], flag_send.at[n], flag_recv.at[n], peer)
        for n, peer in enumerate((along_x, along_y, across, twin))
    ] + [
        remote(flags.at[1], flags_in.at[6 + n], flag_send.at[4 + n], flag_recv.at[4 + n], peer)
        for n, peer in enumerate((along_x, along_y))
    ]
    flags_on = remote(flags_in.at[pl.ds(0, 2)], flags_far, far_sem.at[0], far_sem.at[1], twin)
    for copy in flag_moves:
        copy.start()
    slices = 4
    tall = rows // slices

    panel_moves = [
        remote(
            matrix.at[:, pl.ds(n * LANES, LANES)], panel.at[n], panel_send.at[n], panel_recv.at[n], twin
        )
        for n in range(cols // LANES)
    ]
    def own_panel(n):
        return raw.at[chunks + n // 4, n % 4]

    panel_local = [
        pltpu.make_async_copy(
            matrix.at[:, pl.ds(n * LANES, LANES)], own_panel(n), local_sem.at[2 * chunks + n]
        )
        for n in range(cols // LANES)
    ]
    piece_local = [
        pltpu.make_async_copy(
            matrix.at[:, pl.ds(pl.multiple_of((level * chunks + n) * LANES, LANES), LANES)],
            raw.at[n, 0],
            local_sem.at[n],
        )
        for n in range(chunks)
    ]
    for copy in panel_moves + panel_local + piece_local:
        copy.start()

    def expand(flags, first, width):
        index = lax.broadcasted_iota(jnp.int32, (flags.shape[1], width), 0)
        lane = lax.broadcasted_iota(jnp.int32, (flags.shape[1], width), 1)
        start = (index - first) * block
        table = jnp.where((lane >= start) & (lane < start + block), 1.0, 0.0)
        return jnp.dot(
            flags.astype(jnp.float32).astype(jnp.bfloat16), table.astype(jnp.bfloat16), preferred_element_type=jnp.float32
        )

    per_chunk = LANES // block

    def expand_chunks(flags, store):
        for n in range(chunks):
            store(n, expand(flags, (level * chunks + n) * per_chunk, LANES))

    def store_x(slot):
        def store(n, values):
            flags_x[n, slot] = values
        return store

    def store_lent(k):
        def store(n, values):
            flags_lent_keep[n, k] = values
        return store

    def store_keep(n, values):
        flags_keep[n] = values

    group = 8

    def prepare_panel(side, owner_col):
        for n in range(cols // half):
            owner = owner_col * (cols // rows) + n // 2
            slot = (owner // 2 + y) % 2 * 2 + (owner % 2 + x) % 2
            pair = slot if n % 2 == 0 else slot % 2 * 2 + slot // 2
            left = n % 2 * half

            def body(i, carry):
                base = pl.multiple_of(i * group, group)
                for m in range(half // LANES):
                    lanes = n * half + m * LANES
                    flags = flags_a[side, pl.ds(base, group), lanes : lanes + LANES]
                    for b in range(group):
                        at = pl.ds(pl.multiple_of((i * group + b) * block, block), block)
                        if side:
                            values = panel[lanes // LANES, at, :]
                        else:
                            values = own_panel(lanes // LANES)[at, :]
                        high, low = split(values * flags[b : b + 1])
                        a_high[pair, at, left + m * LANES : left + (m + 1) * LANES] = high
                        a_low[pair, at, left + m * LANES : left + (m + 1) * LANES] = low
                return carry

            lax.fori_loop(0, block_rows // group, body, 0)

    def at_block(i, b):
        return pl.ds(pl.multiple_of((i * group + b) * block, block), block)

    def convert(task, slot, top):
        which = task - (task // chunks) * (task - chunks)

        def body(i, carry):
            flags = flags_x[which, slot, pl.ds(pl.multiple_of(i * group, group), group), :]
            for b in range(group):
                at = at_block(i, b)
                high, low = split(raw[task, slot, at, :] * flags[b : b + 1])
                both[at, 0:LANES] = high
                both[at, LANES : 2 * LANES] = low
            return carry

        steps = block_rows // group // 2
        lax.fori_loop(top * steps, (top + 1) * steps, body, 0)

    def staged(n):
        return raw.at[n, 3]

    def out_move(n, step):
        target = (level + step) % layers
        start = pl.multiple_of((level * chunks + n) * LANES, LANES)
        return remote(
            staged(n).at[pl.ds(pl.multiple_of(target * share, share), share)],
            out.at[:, pl.ds(start, LANES)],
            out_send.at[n, step - 1],
            out_recv.at[n, step - 1],
            {"layer": target},
        )

    def out_local(n):
        start = pl.multiple_of((level * chunks + n) * LANES, LANES)
        return pltpu.make_async_copy(
            staged(n).at[pl.ds(pl.multiple_of(level * share, share), share)],
            out.at[:, pl.ds(start, LANES)],
            local_sem.at[chunks + n],
        )

    def finish_rows(task, second, tile):
        steps = block_rows // group // slices

        def square(i, carry):
            flags = flags_keep[task, pl.ds(pl.multiple_of(i * group, group), group), :]
            for b in range(group):
                at = at_block(i, b)
                summed = total[at, 0:LANES] + total[at, LANES : 2 * LANES]
                raw[task + chunks, 0, at, :] = summed * flags[b : b + 1]
            return carry

        def update(i, carry):
            n = task - chunks
            flags = flags_x[n, 0, pl.ds(pl.multiple_of(i * group, group), group), :]
            for b in range(group):
                at = at_block(i, b)
                summed = total[at, 0:LANES] + total[at, LANES : 2 * LANES]
                raw[n, 3, at, :] = 1.5 * (raw[n, 0, at, :] * flags[b : b + 1]) - factor * summed
            return carry

        lax.fori_loop(tile * steps, (tile + 1) * steps, update if second else square, 0)

    def finish(task, second):
        total[...] = jnp.zeros_like(total)
        first_tile = 1 - level * 2 // layers

        def pair(g, carry):
            other = g % 2 * 2 + g // 2

            @pl.when(g >= 2)
            def _():
                for slot, top, arrival in ((g, 0, g + 1), (other, 1, 4 * g - 7)):
                    remote(
                        part(task, slot, top), part(task, slot, top),
                        send_sem.at[task, arrival], recv_sem.at[task, arrival], along_x,
                    ).wait_recv()

            convert(task, g, 0)
            convert(task, other, 1)

            def product(first, count):
                at = pl.ds(pl.multiple_of(first, count), count)
                value = total[at, :]
                for side in (a_high, a_low):
                    value += jnp.dot(side[g, at, :], both[...], preferred_element_type=jnp.float32)
                total[at, :] = value

            def multiply(i, carry):
                product(i * half, half)
                return carry

            def multiply_last(i, carry):
                tile = (first_tile * (slices // 2) + i) % slices
                product(tile * tall, tall)
                finish_rows(task, second, tile)
                for step in range(1, layers if second else 1):
                    target = (level + step) % layers

                    @pl.when(target * slices // layers == tile)
                    def _():
                        out_move(task - chunks, step).start()

                return carry

            @pl.when(g < 3)
            def _():
                lax.fori_loop(0, 2, multiply, 0)

            @pl.when(g == 3)
            def _():
                lax.fori_loop(0, slices, multiply_last, 0)

            return carry

        lax.fori_loop(0, 4, pair, 0)

        if second:
            out_local(task - chunks).start()

    def prepare_lent():
        for side, owner_col in ((0, col), (1, 1 - col)):
            for n in range(cols // LANES):
                owner = owner_col * (cols // rows) + n * LANES // rows
                slot = (owner // 2 + y) % 2 * 2 + (owner % 2 + x) % 2
                pair = slot if n * LANES // half % 2 == 0 else slot % 2 * 2 + slot // 2
                lanes = n * LANES % rows
                for k in range(2):
                    for b in range(extra // block):
                        flag = (side * 2 + k) * block_rows + k * (block_rows - extra // block) + b
                        at = slice(k * extra + b * block, k * extra + (b + 1) * block)
                        values = from_twin[n, at, :] if side else lent[n, at, :]
                        values = values * panel[n, flag : flag + 1, :]
                        high, low = split(values)
                        lent_high[pair, at, lanes : lanes + LANES] = high
                        lent_low[pair, at, lanes : lanes + LANES] = low

    def square_lent(n):
        total[0 : 2 * extra, :] = jnp.zeros((2 * extra, 2 * LANES), jnp.float32)

        def pair(g, carry):
            other = g % 2 * 2 + g // 2
            convert(n, g, 0)
            convert(n, other, 1)
            value = total[0 : 2 * extra, :]
            for side in (lent_high, lent_low):
                value += jnp.dot(side[g], both[...], preferred_element_type=jnp.float32)
            total[0 : 2 * extra, :] = value
            return carry

        lax.fori_loop(0, 4, pair, 0)
        for k in range(2):
            for b in range(extra // block):
                flag = k * (block_rows - extra // block) + b
                at = slice(k * extra + b * block, k * extra + (b + 1) * block)
                to = k * (rows - extra) + b * block
                summed = total[at, 0:LANES] + total[at, LANES : 2 * LANES]
                raw[n + chunks, 1 + k, to : to + block, :] = summed * flags_lent_keep[n, k, flag : flag + 1, :]

    def prepare_own():
        for copy in panel_local:
            copy.wait()
        prepare_panel(0, col)

    for copy in flag_local:
        copy.wait()
    flags_a[0] = expand(flags_in[4], 0, cols)

    @pl.when(col == 1)
    def _():
        lend_all()
        hand_on(0)
        send_x(1)

    prepare_own()

    @pl.when(col == 0)
    def _():
        lend_all()
        send_x(0)

    expand_chunks(flags_in[4], store_x(0))
    expand_chunks(flags_in[5], store_keep)
    flags_x[chunks] = jnp.ones_like(flags_x[chunks])
    for copy in piece_local:
        copy.wait()

    @pl.when(col == 0)
    def _():
        hand_on(0)
        send_x(1)

    for copy in flag_moves:
        copy.wait_recv()
    flags_a[1] = expand(flags_in[3], 0, cols)
    for slot in (1, 2, 3):
        expand_chunks(flags_in[slot - 1], store_x(slot))
    for copy in panel_moves:
        copy.wait_recv()
    prepare_panel(1, 1 - col)
    flags_on.start()
    flags_on.wait_recv()
    for k in range(2):
        for side, source in ((0, flags_in), (1, flags_far)):
            values = expand(source[k], 0, cols)
            first_row = (side * 2 + k) * block_rows
            for n in range(cols // LANES):
                panel[n, first_row : first_row + block_rows, :] = values[:, n * LANES : (n + 1) * LANES]
        expand_chunks(flags_in[6 + k], store_lent(k))
    finish(0, False)

    def first(task, carry):
        hand_on(task)

        @pl.when(task + 1 < chunks)
        def _():
            send_x(task + 1)

        @pl.when(task + 1 == chunks)
        def _():
            send_f(chunks)

        @pl.when(task + 1 == chunks)
        def _():
            pass_lent()

        finish(task, False)
        return carry

    lax.fori_loop(1, chunks, first, 0)
    lend_twin.wait_recv()
    prepare_lent()
    square_lent(0)

    def second(task, carry):
        hand_on(task)

        @pl.when(task + 1 < tasks)
        def _():
            send_f(task + 1)
            square_lent(task + 1 - chunks)

        finish(task, True)
        return carry

    lax.fori_loop(chunks, tasks, second, 0)
    flags_on.wait_send()

    for copy in flag_moves + panel_moves:
        copy.wait_send()

    def drain(n, carry):
        for arrival in range(8):
            move(n, arrival, in_slot(n, 0)).wait_send()
        for arrival in range(6):
            move(n + chunks, arrival, in_slot(n, 0)).wait_send()
        return carry

    lax.fori_loop(0, chunks, drain, 0)
    for k in range(2):
        for step in range(1, layers):
            lend(k, step, level).wait_send()
    lend_twin.wait_send()

    def drain_out(n, carry):
        for step in range(1, layers):
            out_move(n, step).wait()
        out_local(n).wait()
        return carry

    lax.fori_loop(0, chunks, drain_out, 0)


def fused(matrix, pattern, keep):
    rows, cols = matrix.shape
    layers = lax.axis_size("layer")
    block_rows, block_cols = pattern.shape
    block = rows // block_rows
    chunks = cols // layers // LANES
    tasks = 2 * chunks
    half = rows // 2
    factor = 0.5 * DAMPING / (rows * lax.axis_size("row"))

    vmem = pl.BlockSpec(memory_space=pltpu.VMEM)
    anywhere = pl.BlockSpec(memory_space=pl.ANY)
    dma = pltpu.SemaphoreType.DMA
    return pl.pallas_call(
        functools.partial(kernel, layers, block, factor),
        out_shape=jax.ShapeDtypeStruct((rows // layers, cols), jnp.float32),
        in_specs=[anywhere, anywhere],
        out_specs=vmem,
        scratch_shapes=[
            pltpu.VMEM((tasks, 4, rows, LANES), jnp.float32),
            pltpu.VMEM((cols // LANES, rows, LANES), jnp.float32),
            pltpu.VMEM((4, rows, rows), jnp.bfloat16),
            pltpu.VMEM((4, rows, rows), jnp.bfloat16),
            pltpu.VMEM((rows, 2 * LANES), jnp.bfloat16),
            pltpu.VMEM((rows, 2 * LANES), jnp.float32),
            pltpu.VMEM((8, block_rows, block_cols), jnp.int32),
            pltpu.VMEM((2, block_rows, cols), jnp.float32),
            pltpu.VMEM((chunks + 1, 4, block_rows, LANES), jnp.float32),
            pltpu.VMEM((chunks, block_rows, LANES), jnp.float32),
            pltpu.VMEM((cols // LANES, rows // 4, LANES), jnp.float32),
            pltpu.VMEM((4, rows // 4, rows), jnp.bfloat16),
            pltpu.VMEM((4, rows // 4, rows), jnp.bfloat16),
            pltpu.VMEM((2, block_rows, block_cols), jnp.int32),
            pltpu.VMEM((chunks, 2, block_rows, LANES), jnp.float32),
            dma((tasks, 8)),
            dma((tasks, 8)),
            dma((cols // LANES,)),
            dma((cols // LANES,)),
            dma((6,)),
            dma((6,)),
            dma((2,)),
            dma((chunks, max(layers - 1, 1))),
            dma((chunks, max(layers - 1, 1))),
            dma((2 * chunks + cols // LANES,)),
            dma((2, max(layers - 1, 1))),
            dma((2, max(layers - 1, 1))),
            dma((2,)),
            dma((2,)),
            dma((2,)),
        ],
        compiler_params=pltpu.CompilerParams(
            collective_id=0, has_side_effects=True, vmem_limit_bytes=54_200_000
        ),
    )(matrix, jnp.stack([pattern, keep]))


def local(matrix, pattern, keep):
    rows, cols = matrix.shape
    layers = lax.axis_size("layer")
    block = rows // pattern.shape[0]
    fits = (
        lax.axis_size("row") == 4
        and lax.axis_size("col") == 2
        and cols % (layers * LANES) == 0
        and cols // (layers * LANES) >= 3
        and LANES % block == 0
        and block % 16 == 0
        and rows % (32 * block) == 0
        and rows % (8 * layers) == 0
        and (rows // 2) % LANES == 0
        and rows * cols <= 1 << 21
        and layers in (1, 2, 4)
    )
    return (fused if fits else plain)(matrix, pattern, keep)


def solution(mesh):
    placed = (P("row", "col"), P("row", "col"), P("row", "col"))
    return jax.shard_map(
        local, mesh=mesh, in_specs=placed, out_specs=P(("row", "layer"), "col"), check_vma=False
    )
```
